32 devices in a mesh: wide: 8 (over z, x), narrow: 4 (over y, core).
Axes of the slice: x: 2, y: 2, z: 4, core: 2. Of those that a mesh axis runs over, the one named last changes fastest.
Arguments:
- positions: float32 [3, 4096], P(None, ('wide', 'narrow')), may hold values from -1 to 69, as said below
- noise: float32 [3, 16, 4096], P(None, None, ('wide', 'narrow')), may hold values from -6 to 6
Outputs:
- displacement: float32 [3, 16, 4096], P(None, None, ('wide', 'narrow'))
The draws below stay inside these ranges and needn't reach their ends.
Inputs may be any that keep to these rules, and one draw needn't show every extreme that they name: `positions`: any two particles lie at least 1.2 apart.
All inputs are finite; a program needn't handle non-finite values.
Results may differ from the reference program's by a relative error of at most 0.0003.
Values sent between devices are 32-bit elements; how exact they have to be, the bound alone decides.
A program may use at most 64 MiB of HBM per device.

```python
import math
import jax
import jax.numpy as jnp
from jax import lax

S = 16
ITERS = 3
ROOT_STEPS = 30
PARTICLES = 4096


def draw_positions(key, part):
    sites = jnp.arange(PARTICLES, dtype=jnp.int32)
    lattice = jnp.stack([sites % 32, sites // 32 % 32, sites // 1024]).astype(jnp.float32) * 2.2
    jitter = jax.random.uniform(key, (3, PARTICLES), jnp.float32, -0.5, 0.5)
    return lattice + jitter


def shard_levels(stream_key, shape, cuts, smallest, top_value):
    def one(position, blocks):
        draws = jax.random.uniform(jax.random.fold_in(jax.random.fold_in(stream_key, 6), position), (blocks,), jnp.float32, smallest / len(cuts), top_value / len(cuts))
        return jnp.repeat(jnp.exp(draws), shape[position] // blocks).reshape((-1,) + (1,) * (len(shape) - position - 1))

    factor_of = one(*cuts[0])
    for cut in cuts[1:]:
        factor_of = factor_of * one(*cut)
    return factor_of


def normal_values(stream_key, shape, scale, reach, cuts=(), kind=jnp.bfloat16):
    drawn = scale * jax.random.normal(stream_key, shape, jnp.float32)
    if cuts:
        drawn = drawn * shard_levels(stream_key, shape, cuts, -0.22, 0.18)
    return jnp.clip(drawn, -reach, reach).astype(kind)


def setup_inputs(seed: int = 0) -> dict:
    key_list = jax.random.split(jax.random.key(seed), 3)
    positions = draw_positions(jax.random.fold_in(key_list[2], 71), 0)
    noise = normal_values(key_list[1], (3, S, PARTICLES), 1.0, 6.0, ((2, 32),), jnp.float32)
    return dict(positions=positions, noise=noise)


highest = lax.Precision.HIGHEST

def tile_factors(dist_sq, itself):
    safe_sq = jnp.where(itself, 4.0, dist_sq)
    radial = jnp.sqrt(safe_sq)
    inverse = 1.0 / radial
    far_scalar = 0.75 * inverse + 0.5 * inverse * inverse * inverse
    far_outer = (0.75 * inverse - 1.5 * inverse * inverse * inverse) * inverse * inverse
    near_scalar = 1.0 - 0.28125 * radial
    near_outer = 0.09375 * inverse
    nearby = radial < 2.0
    scalar = jnp.where(itself, 1.0, jnp.where(nearby, near_scalar, far_scalar))
    outer_part = jnp.where(itself, 0.0, jnp.where(nearby, near_outer, far_outer))
    return (scalar, outer_part)

def contract(left, kernel):
    return lax.dot_general(left, kernel, (((1,), (1,)), ((), ())), precision=highest, preferred_element_type=jnp.float32)

def tile_product(row_pos, row_ids, col_pos, col_ids, vectors):
    width = vectors.shape[1]
    delta = row_pos[:, :, None] - col_pos[:, None, :]
    dist_sq = delta[0] * delta[0] + delta[1] * delta[1] + delta[2] * delta[2]
    itself = row_ids[:, None] == col_ids[None, :]
    scalar, outer_part = tile_factors(dist_sq, itself)
    result = []
    for component in range(3):
        diag_kernel = scalar + outer_part * delta[component] * delta[component]
        result.append(contract(vectors[component], diag_kernel))
    for first, second in ((0, 1), (0, 2), (1, 2)):
        cross = outer_part * delta[first] * delta[second]
        both = contract(jnp.concatenate([vectors[second], vectors[first]], axis=0), cross)
        result[first] = result[first] + both[:width]
        result[second] = result[second] + both[width:]
    return jnp.stack(result)

def blocked_product(row_pos, row_ids, col_pos, col_ids, vectors):
    rows = row_pos.shape[1]
    block = math.gcd(rows, 512)

    def row_block(index):
        begin = index * block
        pos_block = lax.dynamic_slice_in_dim(row_pos, begin, block, 1)
        id_block = lax.dynamic_slice_in_dim(row_ids, begin, block, 0)
        return tile_product(pos_block, id_block, col_pos, col_ids, vectors)
    pieces = lax.map(row_block, jnp.arange(rows // block, dtype=jnp.int32))
    return jnp.moveaxis(pieces, 0, 2).reshape(3, vectors.shape[1], rows)

def gram_of(left, right):
    return jnp.einsum('asp,atp->st', left, right, precision=highest)

def stacked_gram(stacked, right):
    return jnp.einsum('kasp,atp->kst', stacked, right, precision=highest)

def stacked_remove(stacked, weights):
    return jnp.einsum('kasp,kst->atp', stacked, weights, precision=highest)

def rotate(block, matrix):
    return jnp.einsum('atp,ts->asp', block, matrix, precision=highest)

def cholesky_pair(gram):
    order = gram.shape[0]
    places = jnp.arange(order, dtype=jnp.int32)
    lower = jnp.zeros((order, order), jnp.float32)
    for column in range(order):
        needed = gram[:, column] - jnp.dot(lower, lower[column, :], precision=highest, preferred_element_type=jnp.float32)
        pivot = jnp.sqrt(needed[column])
        entries = jnp.where(places >= column, needed / pivot, 0.0)
        marker = (places == column).astype(jnp.float32)
        lower = lower + entries[:, None] * marker[None, :]
    solved = jnp.zeros((order, order), jnp.float32)
    for row in range(order):
        marker = (places == row).astype(jnp.float32)
        fresh = (marker - jnp.dot(lower[row, :], solved, precision=highest, preferred_element_type=jnp.float32)) / lower[row, row]
        solved = solved + marker[:, None] * fresh[None, :]
    return (lower.T, solved.T)

def tridiagonal(diagonal_blocks, lower_blocks):
    width = diagonal_blocks[0].shape[0]
    order = len(diagonal_blocks) * width
    matrix = jnp.zeros((order, order), jnp.float32)
    for index, block in enumerate(diagonal_blocks):
        offset = index * width
        matrix = matrix.at[offset:offset + width, offset:offset + width].set(block)
    for index, block in enumerate(lower_blocks):
        offset = index * width
        matrix = matrix.at[offset + width:offset + 2 * width, offset:offset + width].set(block)
        matrix = matrix.at[offset:offset + width, offset + width:offset + 2 * width].set(block.T)
    return matrix

def matrix_root(matrix):
    identity = jnp.eye(matrix.shape[0], dtype=jnp.float32)
    scale = jnp.sqrt(jnp.sum(matrix * matrix))

    def newton(turn, carry):
        current, other = carry
        factor = 1.5 * identity - 0.5 * jnp.dot(other, current, precision=highest, preferred_element_type=jnp.float32)
        return (jnp.dot(current, factor, precision=highest, preferred_element_type=jnp.float32), jnp.dot(factor, other, precision=highest, preferred_element_type=jnp.float32))
    current, other = lax.fori_loop(0, ROOT_STEPS, newton, (matrix / scale, identity))
    return current * jnp.sqrt(scale)

def reference(positions, noise):
    width = noise.shape[1]
    ids = jnp.arange(positions.shape[1], dtype=jnp.int32)
    start_upper, start_inverse = cholesky_pair(gram_of(noise, noise))
    basis = [rotate(noise, start_inverse)]
    diagonal_blocks = []
    lower_blocks = []
    for index in range(ITERS):
        image = blocked_product(positions, ids, positions, ids, basis[index])
        stacked = jnp.stack(basis)
        projections = stacked_gram(stacked, image)
        current_block = projections[-1]
        diagonal_blocks.append(0.5 * (current_block + current_block.T))
        if index + 1 < ITERS:
            work = image - stacked_remove(stacked, projections)
            again = stacked_gram(stacked, work)
            work = work - stacked_remove(stacked, again)
            upper, inverse = cholesky_pair(gram_of(work, work))
            lower_blocks.append(upper)
            basis.append(rotate(work, inverse))
    root = matrix_root(tridiagonal(diagonal_blocks, lower_blocks))
    mixing = jnp.dot(root[:, :width], start_upper, precision=highest, preferred_element_type=jnp.float32).reshape(ITERS, width, width)
    return jnp.einsum('katp,kts->asp', jnp.stack(basis), mixing, precision=highest)
```

```python
import functools

import jax
import jax.numpy as jnp
from jax import lax
from jax.experimental import pallas as pl
from jax.experimental.pallas import tpu as pltpu
from jax.sharding import PartitionSpec as P

ITERS = 3
ROOT_STEPS = 30
HI = lax.Precision.HIGHEST
MESH = pl.DeviceIdType.MESH
CACHE_LIMIT = 40 * 2**20
PAIRS = ((0, 0), (1, 1), (2, 2), (0, 1), (0, 2), (1, 2))


def split3(a):
    h = a.astype(jnp.bfloat16)
    r = a - h.astype(jnp.float32)
    m = r.astype(jnp.bfloat16)
    l = (r - m.astype(jnp.float32)).astype(jnp.bfloat16)
    return h, m, l


def precise(a, b, dims):
    x, y = split3(a), split3(b)

    def d(p, q):
        return lax.dot_general(x[p], y[q], (dims, ((), ())), preferred_element_type=jnp.float32)

    return ((d(0, 2) + d(2, 0)) + d(1, 1)) + (d(0, 1) + d(1, 0)) + d(0, 0)


def nn(a, b):
    return precise(a, b, ((1,), (0,)))


def nt(a, b):
    return precise(a, b, ((1,), (1,)))


def nt_low(a, b):
    return lax.dot_general(
        a, b, (((1,), (1,)), ((), ())), preferred_element_type=jnp.float32
    )


def iota(shape, dim):
    return lax.broadcasted_iota(jnp.int32, shape, dim)


def eliminate(k, aug):
    rows = iota(aug.shape, 0)
    lanes = iota(aug.shape, 1)
    pivot_row = jnp.sum(jnp.where(rows == k, aug, 0.0), axis=0, keepdims=True)
    column = jnp.sum(jnp.where(lanes == k, aug, 0.0), axis=1, keepdims=True)
    pivot = jnp.sum(jnp.where(rows[:, :1] == k, column, 0.0), axis=0, keepdims=True)
    scale = lax.rsqrt(pivot)
    scaled = pivot_row * scale
    return jnp.where(
        rows > k, aug - (column * scale) * scaled, jnp.where(rows == k, scaled, aug)
    )


def body(
    wide,
    narrow,
    width,
    cached,
    pos_ref,
    noise_ref,
    out_ref,
    buf,
    rowpos,
    colpos,
    mh,
    ml,
    acc,
    ssem,
    rsem,
):
    count = wide * narrow
    local = pos_ref.shape[1]
    comp = 3 * width
    slab_at = comp
    pos_at = comp + width
    group = 4
    chunks = count // group
    span = group * local
    w = lax.axis_index("wide")
    n = lax.axis_index("narrow")
    me = w * narrow + n
    ny = narrow // 2
    y, core = lax.div(n, 2), lax.rem(n, 2)
    sibling = (w, y * 2 + 1 - core)
    wide_to = [(lax.rem(w + k, wide), n) for k in range(1, wide)]
    y_to = [(w, lax.rem(y + q, ny) * 2 + core) for q in range(1, ny)]

    barrier = pltpu.get_barrier_semaphore()
    peers = wide_to + y_to + [sibling]
    for peer in peers:
        pl.semaphore_signal(barrier, inc=1, device_id=peer, device_id_type=MESH)

    def exchange(par, begin, size):
        sent = []

        def copy(slot, target, index):
            view = buf.at[par, slot, pl.ds(begin, size)]
            return pltpu.make_async_remote_copy(
                src_ref=view,
                dst_ref=view,
                send_sem=ssem.at[par, index],
                recv_sem=rsem.at[par, slot],
                device_id=target,
                device_id_type=MESH,
            )

        def send(slot, target):
            one = copy(slot, target, len(sent))
            one.start()
            sent.append(one)

        def arrived(slot):
            copy(slot, sibling, 0).wait_recv()

        for target in wide_to:
            send(me, target)
        for target in y_to:
            send(me, target)
        send(me, sibling)
        for k in range(1, wide):
            slot = lax.rem(w + wide - k, wide) * narrow + n
            arrived(slot)
            for target in y_to:
                send(slot, target)
            send(slot, sibling)
        for k in range(wide):
            for q in range(1, ny):
                from_y = lax.rem(y + ny - q, ny) * 2 + core
                slot = lax.rem(w + wide - k, wide) * narrow + from_y
                arrived(slot)
                send(slot, sibling)
        for k in range(wide):
            for q in range(ny):
                from_n = lax.rem(y + ny - q, ny) * 2 + 1 - core
                arrived(lax.rem(w + wide - k, wide) * narrow + from_n)
        for one in sent:
            one.wait_send()

    def put_block(par, rows):
        for c in range(3):
            buf[par, me, c * width : (c + 1) * width, :] = rows[:, c * local : (c + 1) * local]

    def put_slab(par, slab):
        pad = jnp.zeros((width, local - slab.shape[1]), jnp.float32)
        buf[par, me, slab_at : slab_at + width, :] = (
            slab if slab.shape[1] == local else jnp.concatenate([slab, pad], axis=1)
        )

    def slab_sum(par):
        def add(d, total):
            return total + buf[par, d, slab_at : slab_at + width, :]

        return lax.fori_loop(0, count, add, jnp.zeros((width, local), jnp.float32))

    def make_tile(chunk, base):
        for t in range(group):
            col = colpos[chunk * group + t]
            for r in range(local // 16):
                rs = slice(r * 16, r * 16 + 16)
                d = [rowpos[c, rs, :] - col[c : c + 1, :] for c in range(3)]
                d2 = d[0] * d[0] + d[1] * d[1] + d[2] * d[2]
                inv = lax.rsqrt(jnp.maximum(d2, 1.0))
                inv2 = inv * inv
                near = d2 < 4.0
                scalar = jnp.where(near, 1.0 - 0.28125 * (d2 * inv), inv * (0.75 + 0.5 * inv2))
                outer = inv * jnp.where(near, 0.09375, (0.75 - 1.5 * inv2) * inv2)
                od = [outer * x for x in d]
                for m, (a, b) in enumerate(PAIRS):
                    value = od[a] * d[b]
                    if a == b:
                        value = value + scalar
                    high = value.astype(jnp.bfloat16)
                    low = (value - high.astype(jnp.float32)).astype(jnp.bfloat16)
                    at = slice(m * local + r * 16, m * local + r * 16 + 16)
                    mh[base, at, t * local : (t + 1) * local] = high
                    ml[base, at, t * local : (t + 1) * local] = low

    def product(par, fresh, aug):
        acc[...] = jnp.zeros_like(acc)
        per = -(-width // chunks)

        def step(chunk, aug):
            base = chunk if cached else 0
            if fresh or not cached:
                make_tile(chunk, base)
            for extra in range(per):
                k = chunk * per + extra
                aug = jnp.where(k < width, eliminate(k, aug), aug)
            v = jnp.concatenate(
                [buf[par, chunk * group + t, 0:comp, :] for t in range(group)], axis=1
            )
            vh = v.astype(jnp.bfloat16)
            vl = (v - vh.astype(jnp.float32)).astype(jnp.bfloat16)
            fill = jnp.zeros((local - 2 * comp, span), jnp.bfloat16)
            both = jnp.concatenate([vh, vl, fill], axis=0)
            acc[...] += nt_low(mh[base], both)
            acc[...] += nt_low(ml[base], both)
            return aug

        aug = lax.fori_loop(0, chunks, step, aug)
        turned = []
        for m in range(6):
            one = jnp.transpose(acc[m * local : (m + 1) * local, :])
            turned.append(one[0:comp] + one[comp : 2 * comp])
        where = {pair: m for m, pair in enumerate(PAIRS)}
        parts = []
        for a in range(3):
            total = None
            for b in range(3):
                m = where[(min(a, b), max(a, b))]
                piece = turned[m][b * width : (b + 1) * width]
                total = piece if total is None else total + piece
            parts.append(total)
        return jnp.concatenate(parts, axis=1), aug

    def hot(shape, shift):
        return jnp.where(iota(shape, 0) + shift == iota(shape, 1), 1.0, 0.0)

    eye = hot((width, width), 0)

    def augmented(gram):
        return jnp.concatenate([gram, eye], axis=1)

    x = jnp.concatenate([noise_ref[c] for c in range(3)], axis=1)
    put_block(0, x)
    put_slab(0, nt(x, x))
    buf[0, me, pos_at : pos_at + 3, :] = pos_ref[...]
    buf[0, me, pos_at + 3 : pos_at + 8, :] = jnp.zeros((5, local), jnp.float32)
    square = jnp.concatenate(
        [pos_ref[...], jnp.zeros((local - 3, local), jnp.float32)], axis=0
    )
    turned_pos = jnp.transpose(square)
    for c in range(3):
        rowpos[c] = jnp.broadcast_to(turned_pos[:, c : c + 1], (local, local))
    acc[...] = jnp.zeros_like(acc)
    pl.semaphore_wait(barrier, len(peers))
    exchange(0, 0, pos_at + 8)

    def keep(d, carry):
        colpos[d] = buf[0, d, pos_at : pos_at + 8, :]
        return carry

    lax.fori_loop(0, count, keep, 0)
    total = slab_sum(0)
    image, aug = product(0, True, augmented(total[:, 0:width]))
    start_upper, linv = aug[:, 0:width], aug[:, width : 2 * width]
    basis = [nn(linv, x)]
    images = [nn(linv, image)]
    diagonal = []
    lower = []
    for j in range(1, ITERS):
        par = j % 2
        work = images[-1]
        lanes = width * (j + 1 + j * j)
        slab = nt(work, jnp.concatenate(basis + [work], axis=0))
        rows = [slab]
        stacked = jnp.concatenate(basis, axis=0)
        for member in basis:
            rows.append(nt(member, stacked))
        placed = jnp.concatenate(rows, axis=1)
        put_block(par, work)
        put_slab(par, placed)
        exchange(par, 0, pos_at)
        total = slab_sum(par)
        ht = total[:, 0 : width * j]
        square_gram = total[:, width * j : width * (j + 1)]
        at = width * (j + 1)
        gram = jnp.concatenate(
            [total[:, at + width * j * m : at + width * j * (m + 1)] for m in range(j)], axis=0
        )
        again = ht - nn(ht, gram)
        ft = ht + again
        diagonal.append(ht[:, width * (j - 1) : width * j])
        left = nt(ft, ht)
        reduced = square_gram - left - nt(ht, ft) + nt(nn(ft, gram), ft)
        image, aug = product(par, False, augmented(reduced))
        upper, linv = aug[:, 0:width], aug[:, width : 2 * width]
        lower.append(upper)
        basis.append(nn(linv, work - nn(ft, stacked)))
        images.append(nn(linv, image - nn(ft, jnp.concatenate(images, axis=0))))
    par = ITERS % 2
    put_slab(par, nt(images[-1], basis[-1]))
    exchange(par, slab_at, width)
    diagonal.append(slab_sum(par)[:, 0:width])

    order = ITERS * width

    strips = []
    for k in range(ITERS):
        cells = [jnp.zeros((width, width), jnp.float32)] * ITERS
        cells[k] = 0.5 * (diagonal[k] + nt(eye, diagonal[k]))
        if k > 0:
            cells[k - 1] = lower[k - 1]
        if k + 1 < ITERS:
            cells[k + 1] = nt(eye, lower[k])
        strips.append(jnp.concatenate(cells, axis=1))
    matrix = jnp.concatenate(strips, axis=0)
    size = jnp.sum(jnp.sum(matrix * matrix, axis=1, keepdims=True), axis=0, keepdims=True)
    scale = jnp.sqrt(size)
    identity = hot((order, order), 0)

    def newton(turn, carry):
        current, other = carry
        factor = 1.5 * identity - 0.5 * nn(other, current)
        return nn(current, factor), nn(factor, other)

    current, other = lax.fori_loop(0, ROOT_STEPS, newton, (matrix / scale, identity))
    mixing = nn(nt(eye, start_upper), current[0:width, :]) * jnp.sqrt(scale)
    result = nn(mixing, jnp.concatenate(basis, axis=0))
    for c in range(3):
        out_ref[c] = result[:, c * local : (c + 1) * local]


def solution(mesh):
    wide, narrow = mesh.shape["wide"], mesh.shape["narrow"]
    count = wide * narrow

    def per_device(positions, noise):
        width, local = noise.shape[1], noise.shape[2]
        comp = 3 * width
        cached = 6 * local * local * count * 4 <= CACHE_LIMIT
        tiles = count // 4 if cached else 1
        return pl.pallas_call(
            functools.partial(body, wide, narrow, width, cached),
            out_shape=jax.ShapeDtypeStruct(noise.shape, jnp.float32),
            in_specs=[pl.BlockSpec(memory_space=pltpu.VMEM)] * 2,
            out_specs=pl.BlockSpec(memory_space=pltpu.VMEM),
            scratch_shapes=[
                pltpu.VMEM((2, count, comp + width + 8, local), jnp.float32),
                pltpu.VMEM((3, local, local), jnp.float32),
                pltpu.VMEM((count, 8, local), jnp.float32),
                pltpu.VMEM((tiles, 6 * local, 4 * local), jnp.bfloat16),
                pltpu.VMEM((tiles, 6 * local, 4 * local), jnp.bfloat16),
                pltpu.VMEM((6 * local, local), jnp.float32),
                pltpu.SemaphoreType.DMA((2, count)),
                pltpu.SemaphoreType.DMA((2, count)),
            ],
            compiler_params=pltpu.CompilerParams(
                collective_id=0, has_side_effects=True, vmem_limit_bytes=60 * 2**20
            ),
        )(positions, noise)

    return jax.shard_map(
        per_device,
        mesh=mesh,
        in_specs=(P(None, ("wide", "narrow")), P(None, None, ("wide", "narrow"))),
        out_specs=P(None, None, ("wide", "narrow")),
        check_vma=False,
    )
```

```python
import functools

import jax
import jax.numpy as jnp
from jax import lax
from jax.experimental import pallas as pl
from jax.experimental.pallas import tpu as pltpu
from jax.sharding import PartitionSpec as P

ITERS = 3
ROOT_STEPS = 30
HI = lax.Precision.HIGHEST
MESH = pl.DeviceIdType.MESH
CACHE_LIMIT = 50 * 2**20
PAIRS = ((0, 0), (1, 1), (2, 2), (0, 1), (0, 2), (1, 2))


def split3(a):
    h = a.astype(jnp.bfloat16)
    r = a - h.astype(jnp.float32)
    m = r.astype(jnp.bfloat16)
    l = (r - m.astype(jnp.float32)).astype(jnp.bfloat16)
    return h, m, l


def precise(a, b, dims):
    x, y = split3(a), split3(b)

    def d(p, q):
        return lax.dot_general(x[p], y[q], (dims, ((), ())), preferred_element_type=jnp.float32)

    return ((d(0, 2) + d(2, 0)) + d(1, 1)) + (d(0, 1) + d(1, 0)) + d(0, 0)


def nn(a, b):
    return precise(a, b, ((1,), (0,)))


def nt(a, b):
    return precise(a, b, ((1,), (1,)))


def nn_low(a, b):
    return lax.dot_general(
        a, b, (((1,), (0,)), ((), ())), preferred_element_type=jnp.float32
    )


def iota(shape, dim):
    return lax.broadcasted_iota(jnp.int32, shape, dim)


def eliminate(k, aug):
    rows = iota(aug.shape, 0)
    lanes = iota(aug.shape, 1)
    pivot_row = jnp.sum(jnp.where(rows == k, aug, 0.0), axis=0, keepdims=True)
    column = jnp.sum(jnp.where(lanes == k, aug, 0.0), axis=1, keepdims=True)
    pivot = jnp.sum(jnp.where(rows[:, :1] == k, column, 0.0), axis=0, keepdims=True)
    scale = lax.rsqrt(pivot)
    scaled = pivot_row * scale
    return jnp.where(
        rows > k, aug - (column * scale) * scaled, jnp.where(rows == k, scaled, aug)
    )


def body(
    wide,
    narrow,
    width,
    cached,
    pos_ref,
    noise_ref,
    out_ref,
    buf,
    colpos,
    rowpos,
    colcast,
    mh,
    ml,
    vcat,
    stage,
    red,
    sums,
    fin,
    ssem,
    rsem,
):
    local = pos_ref.shape[1]
    comp = 3 * width
    w = lax.axis_index("wide")
    n = lax.axis_index("narrow")
    outer = 4 if wide % 4 == 0 else 1
    inner = wide // outer
    wo, wi = lax.div(w, inner), lax.rem(w, inner)
    outer_at = [lax.rem(wo + k, outer) * inner + wi for k in range(1, outer)]
    inner_at = [wo * inner + lax.rem(wi + k, inner) for k in range(1, inner)]
    wide_at = [lax.rem(w + k, wide) for k in range(1, wide)]
    narrow_at = [lax.rem(n + q, narrow) for q in range(1, narrow)]
    far = (lax.rem(w + 1, wide), n)

    barrier = pltpu.get_barrier_semaphore()
    peers = [(a, n) for a in wide_at] + [(w, b) for b in narrow_at]
    for peer in peers:
        pl.semaphore_signal(barrier, inc=1, device_id=peer, device_id_type=MESH)

    sent = []
    used = [0]
    pos_wide, pos_narrow = 0, wide
    block_at = wide + narrow
    red_at = block_at + ITERS * wide
    sum_at = red_at + ITERS * narrow
    fin_at = sum_at + (ITERS + 1) * narrow

    def make(src, dst, slot, target, index):
        return pltpu.make_async_remote_copy(
            src_ref=src,
            dst_ref=dst,
            send_sem=ssem.at[index],
            recv_sem=rsem.at[slot],
            device_id=target,
            device_id_type=MESH,
        )

    def send(src, dst, slot, target):
        one = make(src, dst, slot, target, used[0])
        used[0] += 1
        one.start()
        sent.append(one)

    def arrived(dst, slot):
        make(dst, dst, slot, far, 0).wait_recv()

    def put_block(e, rows):
        for c in range(3):
            buf[e, w, c * width : (c + 1) * width, :] = rows[:, c * local : (c + 1) * local]

    def padded(slab):
        if slab.shape[1] == local:
            return slab
        pad = jnp.zeros((width, local - slab.shape[1]), jnp.float32)
        return jnp.concatenate([slab, pad], axis=1)

    def gather(e, direct):
        mine = buf.at[e, w]
        for a in wide_at if direct else outer_at + inner_at:
            send(mine, mine, block_at + e * wide + w, (a, n))

    def gathered(e, direct):
        base = block_at + e * wide
        if direct:
            for k in range(1, wide):
                a = lax.rem(w + wide - k, wide)
                arrived(buf.at[e, a], base + a)
            return
        for a in outer_at:
            view = buf.at[e, a]
            arrived(view, base + a)
            for b in inner_at:
                send(view, view, base + a, (b, n))
        for o in range(outer):
            for k in range(1, inner):
                a = lax.rem(wo + o, outer) * inner + lax.rem(wi + k, inner)
                arrived(buf.at[e, a], base + a)

    def spread_sum(e, total):
        sums[e, n] = total
        view = sums.at[e, n]
        for b in narrow_at:
            send(view, view, sum_at + e * narrow + n, (w, b))

    def narrow_sum(e):
        for b in narrow_at:
            arrived(sums.at[e, b], sum_at + e * narrow + b)
        total = sums[e, 0]
        for b in range(1, narrow):
            total = total + sums[e, b]
        return total

    def make_tile(blocks):
        def one(slot, carry):
            square = jnp.concatenate(
                [colpos[slot], jnp.zeros((local - 8, local), jnp.float32)], axis=0
            )
            turned = jnp.transpose(square)
            for c in range(3):
                colcast[c] = jnp.broadcast_to(turned[:, c : c + 1], (local, local))
            for nb, base in blocks:
                row = rowpos[nb]
                for r in range(local // 16):
                    rs = slice(r * 16, r * 16 + 16)
                    d = [row[c : c + 1, :] - colcast[c, rs, :] for c in range(3)]
                    d2 = d[0] * d[0] + d[1] * d[1] + d[2] * d[2]
                    inv = lax.rsqrt(jnp.maximum(d2, 1.0))
                    inv2 = inv * inv
                    near = d2 < 4.0
                    scalar = jnp.where(
                        near, 1.0 - 0.28125 * (d2 * inv), inv * (0.75 + 0.5 * inv2)
                    )
                    part = inv * jnp.where(near, 0.09375, (0.75 - 1.5 * inv2) * inv2)
                    od = [part * x for x in d]
                    at = pl.ds(pl.multiple_of(slot * local + r * 16, 16), 16)
                    for m, (a, b) in enumerate(PAIRS):
                        value = od[a] * d[b]
                        if a == b:
                            value = value + scalar
                        high = value.astype(jnp.bfloat16)
                        low = (value - high.astype(jnp.float32)).astype(jnp.bfloat16)
                        mh[base, at, m * local : (m + 1) * local] = high
                        ml[base, at, m * local : (m + 1) * local] = low
            return carry

        lax.fori_loop(0, wide, one, 0)

    where = {pair: m for m, pair in enumerate(PAIRS)}

    def product(e, solve):
        for slot in range(wide):
            v = buf[e, slot, 0:comp, :]
            vh = v.astype(jnp.bfloat16)
            vcat[0:comp, slot * local : (slot + 1) * local] = vh
            vcat[comp : 2 * comp, slot * local : (slot + 1) * local] = (
                v - vh.astype(jnp.float32)
            ).astype(jnp.bfloat16)
        aug = None
        step = 0
        own = None
        for q in range(1, narrow + 1):
            nb = lax.rem(n + q, narrow)
            if not cached:
                make_tile([(nb, 0)])
            base = nb if cached else 0
            both = nn_low(vcat[...], mh[base])
            result = both[0:comp] + both[comp : 2 * comp] + nn_low(vcat[0:comp, :], ml[base])
            parts = []
            for a in range(3):
                total = None
                for b in range(3):
                    m = where[(min(a, b), max(a, b))]
                    piece = result[b * width : (b + 1) * width, m * local : (m + 1) * local]
                    total = piece if total is None else total + piece
                parts.append(total)
            if q < narrow:
                for a in range(3):
                    stage[e, q, a * width : (a + 1) * width, :] = parts[a]
                send(stage.at[e, q], red.at[e, n], red_at + e * narrow + n, (w, nb))
            else:
                own = parts
            if q == 1:
                aug = solve()
            else:
                upto = -(-width * (q - 1) // (narrow - 1))
                while step < min(upto, width):
                    aug = eliminate(step, aug)
                    step += 1
        for b in narrow_at:
            arrived(red.at[e, b], red_at + e * narrow + b)
            own = [own[a] + red[e, b, a * width : (a + 1) * width, :] for a in range(3)]
        return jnp.concatenate(own, axis=1), aug

    def hot(shape, shift):
        return jnp.where(iota(shape, 0) + shift == iota(shape, 1), 1.0, 0.0)

    eye = hot((width, width), 0)

    def augmented(gram):
        return jnp.concatenate([gram, eye], axis=1)

    def slab_sum(e):
        total = buf[e, 0, comp : comp + width, :]
        for a in range(1, wide):
            total = total + buf[e, a, comp : comp + width, :]
        return total

    places = jnp.concatenate([pos_ref[...], jnp.zeros((5, local), jnp.float32)], axis=0)
    colpos[w] = places
    rowpos[n] = places
    x = jnp.concatenate([noise_ref[c] for c in range(3)], axis=1)
    put_block(0, x)
    buf[0, w, comp : comp + width, :] = padded(nt(x, x))
    pl.semaphore_wait(barrier, len(peers))
    for a in wide_at:
        send(colpos.at[w], colpos.at[w], pos_wide + w, (a, n))
    for b in narrow_at:
        send(rowpos.at[n], rowpos.at[n], pos_narrow + n, (w, b))
    gather(0, True)
    for b in narrow_at:
        arrived(rowpos.at[b], pos_narrow + b)
    for a in wide_at:
        arrived(colpos.at[a], pos_wide + a)
    if cached:
        make_tile([(nb, nb) for nb in range(narrow)])
    gathered(0, True)
    spread_sum(0, slab_sum(0))
    image, aug = product(0, lambda: augmented(narrow_sum(0)[:, 0:width]))
    start_upper, linv = aug[:, 0:width], aug[:, width : 2 * width]
    basis = [nn(linv, x)]
    images = [nn(linv, image)]
    diagonal = []
    lower = []
    for j in range(1, ITERS):
        work = images[-1]
        stacked = jnp.concatenate(basis, axis=0)
        put_block(j, work)
        rows = [nt(work, jnp.concatenate(basis + [work], axis=0))]
        for member in basis:
            rows.append(nt(member, stacked))
        buf[j, w, comp : comp + width, :] = padded(jnp.concatenate(rows, axis=1))
        gather(j, False)
        gathered(j, False)
        spread_sum(j, slab_sum(j))
        kept = {}

        def solve():
            total = narrow_sum(j)
            ht = total[:, 0 : width * j]
            square_gram = total[:, width * j : width * (j + 1)]
            at = width * (j + 1)
            gram = jnp.concatenate(
                [total[:, at + width * j * m : at + width * j * (m + 1)] for m in range(j)],
                axis=0,
            )
            again = ht - nn(ht, gram)
            ft = ht + again
            kept["ft"] = ft
            diagonal.append(ht[:, width * (j - 1) : width * j])
            reduced = square_gram - nt(ft, ht) - nt(ht, ft) + nt(nn(ft, gram), ft)
            return augmented(reduced)

        image, aug = product(j, solve)
        ft = kept["ft"]
        upper, linv = aug[:, 0:width], aug[:, width : 2 * width]
        lower.append(upper)
        basis.append(nn(linv, work - nn(ft, stacked)))
        images.append(nn(linv, image - nn(ft, jnp.concatenate(images, axis=0))))
    fin[w] = padded(nt(images[-1], basis[-1]))
    for a in wide_at:
        send(fin.at[w], fin.at[w], fin_at + w, (a, n))
    for a in wide_at:
        arrived(fin.at[a], fin_at + a)
    total = fin[0]
    for a in range(1, wide):
        total = total + fin[a]
    spread_sum(ITERS, total)
    diagonal.append(narrow_sum(ITERS)[:, 0:width])

    order = ITERS * width

    strips = []
    for k in range(ITERS):
        cells = [jnp.zeros((width, width), jnp.float32)] * ITERS
        cells[k] = 0.5 * (diagonal[k] + nt(eye, diagonal[k]))
        if k > 0:
            cells[k - 1] = lower[k - 1]
        if k + 1 < ITERS:
            cells[k + 1] = nt(eye, lower[k])
        strips.append(jnp.concatenate(cells, axis=1))
    matrix = jnp.concatenate(strips, axis=0)
    size = jnp.sum(jnp.sum(matrix * matrix, axis=1, keepdims=True), axis=0, keepdims=True)
    scale = jnp.sqrt(size)
    identity = hot((order, order), 0)

    def newton(turn, carry):
        current, other = carry
        factor = 1.5 * identity - 0.5 * nn(other, current)
        return nn(current, factor), nn(factor, other)

    current, other = lax.fori_loop(0, ROOT_STEPS, newton, (matrix / scale, identity))
    mixing = nn(nt(eye, start_upper), current[0:width, :]) * jnp.sqrt(scale)
    result = nn(mixing, jnp.concatenate(basis, axis=0))
    for c in range(3):
        out_ref[c] = result[:, c * local : (c + 1) * local]
    for one in sent:
        one.wait_send()


def solution(mesh):
    wide, narrow = mesh.shape["wide"], mesh.shape["narrow"]
    count = wide * narrow

    def per_device(positions, noise):
        width, local = noise.shape[1], noise.shape[2]
        comp = 3 * width
        cached = 6 * local * local * count * 4 <= CACHE_LIMIT
        tiles = narrow if cached else 1
        received = wide + narrow + ITERS * (wide + narrow) + (ITERS + 1) * narrow + wide
        f32 = jnp.float32
        return pl.pallas_call(
            functools.partial(body, wide, narrow, width, cached),
            out_shape=jax.ShapeDtypeStruct(noise.shape, f32),
            in_specs=[pl.BlockSpec(memory_space=pltpu.VMEM)] * 2,
            out_specs=pl.BlockSpec(memory_space=pltpu.VMEM),
            scratch_shapes=[
                pltpu.VMEM((ITERS, wide, comp + width, local), f32),
                pltpu.VMEM((wide, 8, local), f32),
                pltpu.VMEM((narrow, 8, local), f32),
                pltpu.VMEM((3, local, local), f32),
                pltpu.VMEM((tiles, wide * local, 6 * local), jnp.bfloat16),
                pltpu.VMEM((tiles, wide * local, 6 * local), jnp.bfloat16),
                pltpu.VMEM((2 * comp, wide * local), jnp.bfloat16),
                pltpu.VMEM((ITERS, narrow, comp, local), f32),
                pltpu.VMEM((ITERS, narrow, comp, local), f32),
                pltpu.VMEM((ITERS + 1, narrow, width, local), f32),
                pltpu.VMEM((wide, width, local), f32),
                pltpu.SemaphoreType.DMA((2 * received,)),
                pltpu.SemaphoreType.DMA((received,)),
            ],
            compiler_params=pltpu.CompilerParams(
                collective_id=0, has_side_effects=True, vmem_limit_bytes=60 * 2**20
            ),
        )(positions, noise)

    return jax.shard_map(
        per_device,
        mesh=mesh,
        in_specs=(P(None, ("wide", "narrow")), P(None, None, ("wide", "narrow"))),
        out_specs=P(None, None, ("wide", "narrow")),
        check_vma=False,
    )
```

```python
import functools

import jax
import jax.numpy as jnp
from jax import lax
from jax.experimental import pallas as pl
from jax.experimental.pallas import tpu as pltpu
from jax.sharding import PartitionSpec as P

ITERS = 3
ROOT_STEPS = 30
HI = lax.Precision.HIGHEST
MESH = pl.DeviceIdType.MESH
CACHE_LIMIT = 50 * 2**20
PAIRS = ((0, 0), (1, 1), (2, 2), (0, 1), (0, 2), (1, 2))


def split3(a):
    h = a.astype(jnp.bfloat16)
    r = a - h.astype(jnp.float32)
    m = r.astype(jnp.bfloat16)
    l = (r - m.astype(jnp.float32)).astype(jnp.bfloat16)
    return h, m, l


def precise(a, parts, dims):
    rows = a.shape[0]
    left = split3(a)
    yh, ym, yl = parts

    def d(p, q):
        return lax.dot_general(p, q, (dims, ((), ())), preferred_element_type=jnp.float32)

    first = d(jnp.concatenate(left, axis=0), yh)
    second = d(jnp.concatenate(left[:2], axis=0), ym)
    third = d(left[0], yl)
    small = (third + first[2 * rows :]) + second[rows:]
    return (small + (second[:rows] + first[rows : 2 * rows])) + first[:rows]


def nn(a, b):
    return precise(a, split3(b), ((1,), (0,)))


def nt(a, b):
    return precise(a, split3(b), ((1,), (1,)))


def nn_low(a, b):
    return lax.dot_general(
        a, b, (((1,), (0,)), ((), ())), preferred_element_type=jnp.float32
    )


def iota(shape, dim):
    return lax.broadcasted_iota(jnp.int32, shape, dim)


def eliminate(k, aug):
    rows = iota(aug.shape, 0)
    lanes = iota(aug.shape, 1)
    pivot_row = jnp.sum(jnp.where(rows == k, aug, 0.0), axis=0, keepdims=True)
    column = jnp.sum(jnp.where(lanes == k, aug, 0.0), axis=1, keepdims=True)
    pivot = jnp.sum(jnp.where(rows[:, :1] == k, column, 0.0), axis=0, keepdims=True)
    scale = lax.rsqrt(pivot)
    scaled = pivot_row * scale
    return jnp.where(
        rows > k, aug - (column * scale) * scaled, jnp.where(rows == k, scaled, aug)
    )


def body(
    wide,
    narrow,
    width,
    cached,
    pos_ref,
    noise_ref,
    out_ref,
    buf,
    colpos,
    rowpos,
    colcast,
    mh,
    ml,
    vcat,
    stage,
    red,
    sums,
    fin,
    ssem,
    rsem,
):
    local = pos_ref.shape[1]
    comp = 3 * width
    w = lax.axis_index("wide")
    n = lax.axis_index("narrow")
    wide_at = [lax.rem(w + k, wide) for k in range(1, wide)]
    narrow_at = [lax.rem(n + q, narrow) for q in range(1, narrow)]
    far = (lax.rem(w + 1, wide), n)

    barrier = pltpu.get_barrier_semaphore()
    peers = [(a, n) for a in wide_at] + [(w, b) for b in narrow_at]
    for peer in peers:
        pl.semaphore_signal(barrier, inc=1, device_id=peer, device_id_type=MESH)

    sent = []
    used = [0]
    pos_wide, pos_narrow = 0, wide
    block_at = wide + narrow
    red_at = block_at + ITERS * wide
    sum_at = red_at + ITERS * narrow
    fin_at = sum_at + (ITERS + 1) * narrow

    def make(src, dst, slot, target, index):
        return pltpu.make_async_remote_copy(
            src_ref=src,
            dst_ref=dst,
            send_sem=ssem.at[index],
            recv_sem=rsem.at[slot],
            device_id=target,
            device_id_type=MESH,
        )

    def send(src, dst, slot, target):
        one = make(src, dst, slot, target, used[0])
        used[0] += 1
        one.start()
        sent.append(one)

    def arrived(dst, slot):
        make(dst, dst, slot, far, 0).wait_recv()

    def put_block(e, rows):
        for c in range(3):
            buf[e, w, c * width : (c + 1) * width, :] = rows[:, c * local : (c + 1) * local]

    def padded(slab):
        if slab.shape[1] == local:
            return slab
        pad = jnp.zeros((width, local - slab.shape[1]), jnp.float32)
        return jnp.concatenate([slab, pad], axis=1)

    def gather(e):
        mine = buf.at[e, w]
        for a in wide_at:
            send(mine, mine, block_at + e * wide + w, (a, n))

    def gathered(e):
        for a in reversed(wide_at):
            arrived(buf.at[e, a], block_at + e * wide + a)

    def add_narrow(e, slab):
        sums[e, n] = padded(slab)
        view = sums.at[e, n]
        for b in narrow_at:
            send(view, view, sum_at + e * narrow + n, (w, b))

    def add_wide(e):
        for b in narrow_at:
            arrived(sums.at[e, b], sum_at + e * narrow + b)
        total = sums[e, 0]
        for b in range(1, narrow):
            total = total + sums[e, b]
        fin[e, w] = total
        view = fin.at[e, w]
        for a in wide_at:
            send(view, view, fin_at + e * wide + w, (a, n))

    def added(e):
        for a in reversed(wide_at):
            arrived(fin.at[e, a], fin_at + e * wide + a)
        total = fin[e, 0]
        for a in range(1, wide):
            total = total + fin[e, a]
        return total

    def make_tile(single):
        def one(slot, carry):
            square = jnp.concatenate(
                [colpos[slot], jnp.zeros((local - 8, local), jnp.float32)], axis=0
            )
            turned = jnp.transpose(square)
            for c in range(3):
                colcast[c] = jnp.broadcast_to(turned[:, c : c + 1], (local, local))
            def block(index, inner_carry):
                nb = index if cached else single
                base = index if cached else 0
                row = rowpos[nb]
                for r in range(local // 16):
                    rs = slice(r * 16, r * 16 + 16)
                    d = [row[c : c + 1, :] - colcast[c, rs, :] for c in range(3)]
                    d2 = d[0] * d[0] + d[1] * d[1] + d[2] * d[2]
                    inv = lax.rsqrt(jnp.maximum(d2, 1.0))
                    inv2 = inv * inv
                    near = d2 < 4.0
                    scalar = jnp.where(
                        near, 1.0 - 0.28125 * (d2 * inv), inv * (0.75 + 0.5 * inv2)
                    )
                    part = inv * jnp.where(near, 0.09375, (0.75 - 1.5 * inv2) * inv2)
                    od = [part * x for x in d]
                    at = pl.ds(pl.multiple_of(slot * local + r * 16, 16), 16)
                    for m, (a, b) in enumerate(PAIRS):
                        value = od[a] * d[b]
                        if a == b:
                            value = value + scalar
                        high = value.astype(jnp.bfloat16)
                        low = (value - high.astype(jnp.float32)).astype(jnp.bfloat16)
                        mh[base, at, m * local : (m + 1) * local] = high
                        ml[base, at, m * local : (m + 1) * local] = low
                return inner_carry

            lax.fori_loop(0, narrow if cached else 1, block, 0)
            return carry

        lax.fori_loop(0, wide, one, 0)

    where = {pair: m for m, pair in enumerate(PAIRS)}

    def product(e, solve):
        for slot in range(wide):
            v = buf[e, slot, 0:comp, :]
            vh = v.astype(jnp.bfloat16)
            vcat[0:comp, slot * local : (slot + 1) * local] = vh
            vcat[comp : 2 * comp, slot * local : (slot + 1) * local] = (
                v - vh.astype(jnp.float32)
            ).astype(jnp.bfloat16)
        aug = None
        step = 0
        own = None
        for q in range(1, narrow + 1):
            nb = lax.rem(n + q, narrow)
            if not cached:
                make_tile(nb)
            base = nb if cached else 0
            both = nn_low(vcat[...], mh[base])
            result = both[0:comp] + both[comp : 2 * comp] + nn_low(vcat[0:comp, :], ml[base])
            parts = []
            for a in range(3):
                total = None
                for b in range(3):
                    m = where[(min(a, b), max(a, b))]
                    piece = result[b * width : (b + 1) * width, m * local : (m + 1) * local]
                    total = piece if total is None else total + piece
                parts.append(total)
            if q < narrow:
                for a in range(3):
                    stage[e, q, a * width : (a + 1) * width, :] = parts[a]
                send(stage.at[e, q], red.at[e, n], red_at + e * narrow + n, (w, nb))
            else:
                own = parts
            if q == 1:
                aug = solve()
            else:
                upto = -(-width * (q - 1) // (narrow - 1))
                while step < min(upto, width):
                    aug = eliminate(step, aug)
                    step += 1
        for b in narrow_at:
            arrived(red.at[e, b], red_at + e * narrow + b)
            own = [own[a] + red[e, b, a * width : (a + 1) * width, :] for a in range(3)]
        return jnp.concatenate(own, axis=1), aug

    def hot(shape, shift):
        return jnp.where(iota(shape, 0) + shift == iota(shape, 1), 1.0, 0.0)

    eye = hot((width, width), 0)

    def augmented(gram):
        return jnp.concatenate([gram, eye], axis=1)

    places = jnp.concatenate([pos_ref[...], jnp.zeros((5, local), jnp.float32)], axis=0)
    colpos[w] = places
    rowpos[n] = places
    x = jnp.concatenate([noise_ref[c] for c in range(3)], axis=1)
    put_block(0, x)
    pl.semaphore_wait(barrier, len(peers))
    for a in wide_at:
        send(colpos.at[w], colpos.at[w], pos_wide + w, (a, n))
    for b in narrow_at:
        send(rowpos.at[n], rowpos.at[n], pos_narrow + n, (w, b))
    gather(0)
    add_narrow(0, nt(x, x))
    for b in narrow_at:
        arrived(rowpos.at[b], pos_narrow + b)
    add_wide(0)
    for a in wide_at:
        arrived(colpos.at[a], pos_wide + a)
    if cached:
        make_tile(None)
    gathered(0)
    image, aug = product(0, lambda: augmented(added(0)[:, 0:width]))
    start_upper, linv = aug[:, 0:width], aug[:, width : 2 * width]
    basis = [nn(linv, x)]
    images = [nn(linv, image)]
    diagonal = []
    lower = []
    for j in range(1, ITERS):
        work = images[-1]
        stacked = jnp.concatenate(basis, axis=0)
        put_block(j, work)
        gather(j)
        rows = [nt(work, jnp.concatenate(basis + [work], axis=0))]
        for member in basis:
            rows.append(nt(member, stacked))
        add_narrow(j, jnp.concatenate(rows, axis=1))
        add_wide(j)
        gathered(j)
        kept = {}

        def solve():
            total = added(j)
            ht = total[:, 0 : width * j]
            square_gram = total[:, width * j : width * (j + 1)]
            at = width * (j + 1)
            gram = jnp.concatenate(
                [total[:, at + width * j * m : at + width * j * (m + 1)] for m in range(j)],
                axis=0,
            )
            again = ht - nn(ht, gram)
            ft = ht + again
            kept["ft"] = ft
            diagonal.append(ht[:, width * (j - 1) : width * j])
            reduced = square_gram - nt(ft, ht) - nt(ht, ft) + nt(nn(ft, gram), ft)
            return augmented(reduced)

        image, aug = product(j, solve)
        ft = kept["ft"]
        upper, linv = aug[:, 0:width], aug[:, width : 2 * width]
        lower.append(upper)
        basis.append(nn(linv, work - nn(ft, stacked)))
        images.append(nn(linv, image - nn(ft, jnp.concatenate(images, axis=0))))
    add_narrow(ITERS, nt(images[-1], basis[-1]))
    add_wide(ITERS)
    diagonal.append(added(ITERS)[:, 0:width])

    order = ITERS * width

    strips = []
    for k in range(ITERS):
        cells = [jnp.zeros((width, width), jnp.float32)] * ITERS
        cells[k] = 0.5 * (diagonal[k] + nt(eye, diagonal[k]))
        if k > 0:
            cells[k - 1] = lower[k - 1]
        if k + 1 < ITERS:
            cells[k + 1] = nt(eye, lower[k])
        strips.append(jnp.concatenate(cells, axis=1))
    matrix = jnp.concatenate(strips, axis=0)
    size = jnp.sum(jnp.sum(matrix * matrix, axis=1, keepdims=True), axis=0, keepdims=True)
    scale = jnp.sqrt(size)
    identity = hot((order, order), 0)

    def newton(turn, carry):
        both, top = carry
        factor = split3(1.5 * identity - 0.5 * both)
        turned = precise(jnp.concatenate([both, top], axis=0), factor, ((1,), (0,)))
        return precise(turned[0:order], factor, ((1,), (0,))), turned[order:]

    start = matrix / scale
    both, top = lax.fori_loop(0, ROOT_STEPS, newton, (start, start[0:width, :]))
    mixing = nn(nt(eye, start_upper), top) * jnp.sqrt(scale)
    result = nn(mixing, jnp.concatenate(basis, axis=0))
    for c in range(3):
        out_ref[c] = result[:, c * local : (c + 1) * local]
    for one in sent:
        one.wait_send()


def solution(mesh):
    wide, narrow = mesh.shape["wide"], mesh.shape["narrow"]
    count = wide * narrow

    def per_device(positions, noise):
        width, local = noise.shape[1], noise.shape[2]
        comp = 3 * width
        cached = 6 * local * local * count * 4 <= CACHE_LIMIT
        tiles = narrow if cached else 1
        received = (2 * ITERS + 2) * (wide + narrow)
        f32 = jnp.float32
        return pl.pallas_call(
            functools.partial(body, wide, narrow, width, cached),
            out_shape=jax.ShapeDtypeStruct(noise.shape, f32),
            in_specs=[pl.BlockSpec(memory_space=pltpu.VMEM)] * 2,
            out_specs=pl.BlockSpec(memory_space=pltpu.VMEM),
            scratch_shapes=[
                pltpu.VMEM((ITERS, wide, comp, local), f32),
                pltpu.VMEM((wide, 8, local), f32),
                pltpu.VMEM((narrow, 8, local), f32),
                pltpu.VMEM((3, local, local), f32),
                pltpu.VMEM((tiles, wide * local, 6 * local), jnp.bfloat16),
                pltpu.VMEM((tiles, wide * local, 6 * local), jnp.bfloat16),
                pltpu.VMEM((2 * comp, wide * local), jnp.bfloat16),
                pltpu.VMEM((ITERS, narrow, comp, local), f32),
                pltpu.VMEM((ITERS, narrow, comp, local), f32),
                pltpu.VMEM((ITERS + 1, narrow, width, local), f32),
                pltpu.VMEM((ITERS + 1, wide, width, local), f32),
                pltpu.SemaphoreType.DMA((received,)),
                pltpu.SemaphoreType.DMA((received,)),
            ],
            compiler_params=pltpu.CompilerParams(
                collective_id=0, has_side_effects=True, vmem_limit_bytes=60 * 2**20
            ),
        )(positions, noise)

    return jax.shard_map(
        per_device,
        mesh=mesh,
        in_specs=(P(None, ("wide", "narrow")), P(None, None, ("wide", "narrow"))),
        out_specs=P(None, None, ("wide", "narrow")),
        check_vma=False,
    )
```
